256 devices in a mesh: band: 16 (over y, z_lo, core), shard: 16 (over z_hi, x).
Axes of the slice: x: 4, y: 4, z: 8 (z_hi: 4, z_lo: 2; z = z_hi * 2 + z_lo), core: 2. Of those that a mesh axis runs over, the one named last changes fastest.
Arguments:
- activations: bfloat16 [1024, 2304], P('shard'), may hold values from -6 to 6
- encoder: bfloat16 [2304, 131072], P(None, ('band', 'shard')), may hold values from -0.125 to 0.125
- encoder_bias: float32 [131072], P(('band', 'shard')), may hold values from -1 to -0.25
- decoder: bfloat16 [131072, 2304], P(('band', 'shard')), may hold values from -0.125 to 0.125
Outputs:
- losses: float32 [16], replicated
- encoder_grad: bfloat16 [2304, 131072], P(None, ('band', 'shard'))
- decoder_grad: bfloat16 [131072, 2304], P(('band', 'shard'))
The draws below stay inside these ranges and needn't reach their ends.
All inputs are finite; a program needn't handle non-finite values.
Results may differ from the reference program's by a relative error of at most 0.006.
Values may be sent and summed in bfloat16 or wider, within the bound.
No kernel may reach another device: no remote copies, remote signals or barrier semaphores. Data moves between devices by JAX's collectives and lax.ppermute only.
A program may use at most 128 MiB of HBM per device.

```python
import jax
import jax.numpy as jnp
from jax import lax

D = 2304
LATENTS = 131072
ROWS = 1024
N_BAND = 16


def block_levels(key, extent, cuts, least, top_value):
    factor_of = 1.0
    for position, shards_of in cuts:
        steps = jax.random.uniform(jax.random.fold_in(jax.random.fold_in(key, 6), position), (shards_of,), jnp.float32, least / len(cuts), top_value / len(cuts))
        factor_of = factor_of * jnp.repeat(jnp.exp(steps), extent[position] // shards_of).reshape((-1,) + (1,) * (len(extent) - 1 - position))
    return factor_of


def bell_draw(key, shape, scale, most, pieces=(), held_as=jnp.bfloat16):
    loudness = block_levels(key, shape, pieces, -0.22, 0.18) if pieces else 1.0
    array = jax.random.normal(key, shape, jnp.float32) * scale * loudness
    return jnp.minimum(jnp.maximum(array, -most), most).astype(held_as)


def setup_inputs(seed: int = 0) -> dict:
    splits = jax.random.split(jax.random.key(seed), 5)
    activations = bell_draw(splits[0], (ROWS, D), 1.0, 6.0, ((0, 16),))
    encoder = bell_draw(splits[1], (D, LATENTS), D ** -0.5, 0.125, ((1, 256),))
    encoder_bias = jnp.clip(-1.0 + 0.75 * jax.random.uniform(splits[2], (LATENTS,), jnp.float32) ** block_levels(splits[2], (LATENTS,), ((0, 256),), -0.2, 0.2), -1.0, -0.25)
    decoder = bell_draw(splits[3], (LATENTS, D), D ** -0.5, 0.125, ((0, 256),))
    return {"activations": activations, "encoder": encoder, "encoder_bias": encoder_bias, "decoder": decoder}


def reference(activations, encoder, encoder_bias, decoder):
    band_count = N_BAND
    width = LATENTS // band_count
    enc_bands = encoder.reshape(D, band_count, width).transpose(1, 0, 2)
    bias_bands = encoder_bias.reshape(band_count, width)
    dec_bands = decoder.reshape(band_count, width, D)

    def forward(items):
        weight, bias, back = items
        preact = jnp.dot(activations, weight, preferred_element_type=jnp.float32) + bias
        linear = jnp.maximum(preact, 0.0)
        active = (linear * linear).astype(jnp.bfloat16)
        part = jnp.dot(active, back, preferred_element_type=jnp.float32)
        return active, linear, part

    active, linears, parts = lax.map(forward, (enc_bands, bias_bands, dec_bands))
    recon = jnp.cumsum(parts, axis=0)
    errors = activations.astype(jnp.float32)[None] - recon
    losses = jnp.sum(errors * errors, axis=(1, 2)) / (ROWS * D)
    suffix = jnp.flip(jnp.cumsum(jnp.flip(errors, 0), axis=0), 0)
    upstream = (-suffix / band_count).astype(jnp.bfloat16)

    def backward(items):
        acted, linear, back, grad = items
        act_grads = jnp.dot(grad, back.T, preferred_element_type=jnp.float32)
        pre_grads = (2.0 * linear * act_grads).astype(jnp.bfloat16)
        enc_grad = jnp.dot(activations.T, pre_grads, preferred_element_type=jnp.float32).astype(jnp.bfloat16)
        dec_grad = jnp.dot(acted.T, grad, preferred_element_type=jnp.float32).astype(jnp.bfloat16)
        return enc_grad, dec_grad

    enc_grads, dec_grads = lax.map(backward, (active, linears, dec_bands, upstream))
    encoder_grad = enc_grads.transpose(1, 0, 2).reshape(D, LATENTS)
    decoder_grad = dec_grads.reshape(LATENTS, D)
    return (losses, encoder_grad, decoder_grad)
```

```python
import jax
import jax.numpy as jnp
from jax import lax
from jax.experimental import pallas as pl
from jax.experimental.pallas import tpu as pltpu
from jax.sharding import Mesh, PartitionSpec as P

BF = jnp.bfloat16
F32 = jnp.float32
NAMES = ("y", "zl", "core", "zh", "x")
BAND = ("y", "zl", "core")
SHARD = ("zh", "x")
N = 4
BANDS = 16
LANES = 128
DOWN = 1408
UP = 1536
MIX = BF


def pull(value, axis, step):
    return lax.ppermute(value, axis, [(i, (i - step) % N) for i in range(N)])


def swap_core(value):
    return lax.ppermute(value, "core", [(0, 1), (1, 0)])


def pull_by_core(value, axis):
    perm = []
    for i in range(N):
        perm.append((i, (i - 1) % N))
        perm.append((N + i, N + (i + 1) % N))
    return lax.ppermute(value, ("core", axis), perm)


def gather_by_core(value, axis, core):
    half = value.shape[0] // 2
    near = pull_by_core(value, axis)
    far = pull_by_core(lax.dynamic_slice_in_dim(near, core * half, half, 0), axis)
    other = swap_core(near)
    far_other = swap_core(far)
    first = core == 0
    plus = jnp.where(first, near, other)
    minus = jnp.where(first, other, near)
    two = jnp.concatenate([jnp.where(first, far, far_other), jnp.where(first, far_other, far)], 0)
    return [value, plus, two, minus]


def gather_ring(value, axis):
    half = value.shape[0] // 2
    plus = pull(value, axis, 1)
    minus = pull(value, axis, -1)
    far_a = pull(plus[:half], axis, 1)
    far_b = pull(minus[half:], axis, -1)
    return [[value], [plus], [far_a, far_b], [minus]]


def reduce_ring(blocks, axis):
    own, plus, two, minus = blocks
    half = own.shape[0] // 2
    far_a = pull(two[:half].astype(BF), axis, -1)
    far_b = pull(two[half:].astype(BF), axis, 1)
    plus = jnp.concatenate([plus[:half] + far_a.astype(F32), plus[half:]], 0).astype(BF)
    minus = jnp.concatenate([minus[:half], minus[half:] + far_b.astype(F32)], 0).astype(BF)
    return own, pull(plus, axis, -1), pull(minus, axis, 1)


def add_up(terms):
    return terms[0] + terms[1].astype(F32) + terms[2].astype(F32)


def vmem(count):
    return [pl.BlockSpec(memory_space=pltpu.VMEM)] * count


def deal_kernel(a_ref, a1_ref, a2_ref, b_ref, b1_ref, b2_ref, dealt_ref):
    wide = dealt_ref.shape[2]
    cut = a_ref.shape[1] - wide
    part_a = a_ref[...] + a1_ref[...].astype(F32) + a2_ref[...].astype(F32)
    part_b = b_ref[...] + b1_ref[...].astype(F32) + b2_ref[...].astype(F32)
    part_a = part_a.astype(dealt_ref.dtype)
    part_b = part_b.astype(dealt_ref.dtype)
    for k in range(BANDS // 2):
        dealt_ref[2 * k] = part_a[8 * k : 8 * k + 8, :wide]
        dealt_ref[2 * k + 1, :, :cut] = part_a[8 * k : 8 * k + 8, wide:]
        dealt_ref[2 * k + 1, :, cut:] = part_b[8 * k : 8 * k + 8]


def band_kernel(mixed_ref, local_ref, up_ref):
    wide = local_ref.shape[1]
    lane = lax.broadcasted_iota(jnp.int32, (1, LANES), 1)
    found = jnp.zeros((1, LANES), F32)
    error = local_ref[...].astype(F32)
    suffix = jnp.zeros_like(error)
    errors = []
    for k in range(BANDS):
        error = error - mixed_ref[k].astype(F32)
        errors.append(error)
        found = jnp.where(lane == k, jnp.sum(error * error), found)
    for k in reversed(range(BANDS)):
        suffix = suffix + errors[k]
        up_ref[k, :, :wide] = (suffix * (-1.0 / BANDS)).astype(BF)
    high = found.astype(BF).astype(F32)
    low = found - high
    row = lax.broadcasted_iota(jnp.int32, (8, LANES), 0)
    extra = jnp.where(row == 0, high, jnp.where(row == 1, low, 0.0)).astype(BF)
    for k in range(BANDS):
        up_ref[k, :, wide:] = extra


def sort_kernel(mixed_ref, up_a_ref, up_b_ref):
    wide = mixed_ref.shape[2] - LANES
    cut = UP - wide
    rest = 2 * wide - UP
    found = jnp.zeros((1, LANES), F32)
    for k in range(BANDS // 2):
        rows = pl.ds(8 * k, 8)
        up_a_ref[rows, :wide] = mixed_ref[2 * k, :, :wide]
        up_a_ref[rows, wide:] = mixed_ref[2 * k + 1, :, :cut]
        up_b_ref[rows, :rest] = mixed_ref[2 * k + 1, :, cut:wide]
        up_b_ref[rows, rest:] = jnp.zeros((8, LANES), BF)
    for k in range(BANDS):
        found = found + jnp.sum(mixed_ref[k, :, wide:].astype(F32), axis=0, keepdims=True)
    high = found.astype(BF).astype(F32)
    low = found - high
    row = lax.broadcasted_iota(jnp.int32, (8, LANES), 0)
    up_b_ref[:8, rest:] = jnp.where(row == 0, high, jnp.where(row == 1, low, 0.0)).astype(BF)


def lay(pieces, shape):
    def kernel(*refs):
        for source, (_, row, rows, columns, to_row, to_column) in zip(refs, pieces):
            refs[-1][to_row : to_row + rows, to_column : to_column + columns] = source[row : row + rows, :columns]

    return pl.pallas_call(
        kernel,
        out_shape=jax.ShapeDtypeStruct(shape, BF),
        in_specs=vmem(len(pieces)),
        out_specs=vmem(1)[0],
    )(*[p[0] for p in pieces])


def on_device(activations, encoder, encoder_bias, decoder):
    rows, width = activations.shape
    block = rows * N
    divisor = block * N * width
    core = lax.axis_index("core")
    band = lax.axis_index(BAND)

    column = jnp.concatenate(gather_by_core(activations, "zh", core), 0)
    held = gather_by_core(column, "x", core)

    linears, actives, terms = [], [], []
    for part in held:
        preact = jnp.dot(part, encoder, preferred_element_type=F32) + encoder_bias
        linear = jnp.maximum(preact, 0.0)
        active = (linear * linear).astype(BF)
        linears.append(linear)
        actives.append(active)
        terms.append(jnp.dot(active, decoder, preferred_element_type=F32))

    part_a = add_up(reduce_ring([t[:, :DOWN] for t in terms], "x"))
    part_a = reduce_ring([part_a[o * rows : (o + 1) * rows] for o in range(N)], "zh")
    part_b = add_up(
        reduce_ring(
            [jnp.concatenate([t[o * rows : (o + 1) * rows, DOWN:] for t in terms], 0) for o in range(N)], "zh"
        )
    )
    part_b = reduce_ring([part_b[o * rows : (o + 1) * rows] for o in range(N)], "x")

    wide = width // 2
    dealt = pl.pallas_call(
        deal_kernel,
        out_shape=jax.ShapeDtypeStruct((BANDS, 8, wide), MIX),
        in_specs=vmem(6),
        out_specs=vmem(1)[0],
    )(*part_a, *part_b)
    mixed = lax.all_to_all(dealt, BAND, 0, 0)
    local = lax.dynamic_slice(activations, (8 * (band // 2), wide * (band % 2)), (8, wide))
    ups = pl.pallas_call(
        band_kernel,
        out_shape=jax.ShapeDtypeStruct((BANDS, 8, wide + LANES), BF),
        in_specs=vmem(2),
        out_specs=vmem(1)[0],
    )(mixed, local)
    ups = lax.all_to_all(ups, BAND, 0, 0)
    rest = width - UP
    up_a, up_b = pl.pallas_call(
        sort_kernel,
        out_shape=[jax.ShapeDtypeStruct((rows, UP), BF), jax.ShapeDtypeStruct((rows, rest + LANES), BF)],
        in_specs=vmem(1),
        out_specs=vmem(2),
    )(ups)

    up_a = jnp.concatenate(sum(gather_ring(up_a, "zh"), []), 0)
    up_a = gather_ring(up_a, "x")
    up_b = jnp.concatenate(sum(gather_ring(up_b, "x"), []), 0)
    up_b = gather_ring(up_b, "zh")
    pieces, found = [], 0.0
    for i in range(N):
        start = i * block
        for piece in up_a[i]:
            pieces.append((piece, 0, piece.shape[0], UP, start, 0))
            start += piece.shape[0]
        at = 0
        for piece in up_b[i]:
            for o in range(piece.shape[0] // rows):
                pieces.append((piece, o * rows, rows, rest, (at + o) * block + i * rows, UP))
            at += piece.shape[0] // rows
            found = found + jnp.sum(piece[:, rest:].astype(F32), axis=0)
    losses = found[:BANDS] / divisor
    up = lay(pieces, (block * N, width))

    gathered = jnp.concatenate(held, 0)
    linear = jnp.concatenate(linears, 0)
    active = jnp.concatenate(actives, 0)
    gathered, linear, active = lax.optimization_barrier((gathered, linear, active))
    act_grads = jnp.einsum("rd,ld->rl", up, decoder, preferred_element_type=F32)
    dec_grads = jnp.einsum("rl,rd->ld", active, up, preferred_element_type=F32)
    pre_grads = (2.0 * linear * act_grads).astype(BF)
    enc_grads = jnp.einsum("rd,rl->dl", gathered, pre_grads, preferred_element_type=F32)
    return losses, enc_grads.astype(BF), dec_grads.astype(BF)


def solution(mesh):
    grid = Mesh(mesh.devices.reshape(4, 2, 2, 4, 4), NAMES)
    both = BAND + SHARD
    return jax.shard_map(
        on_device,
        mesh=grid,
        in_specs=(P(SHARD, None), P(None, both), P(both), P(both, None)),
        out_specs=(P(), P(None, both), P(both, None)),
        check_vma=False,
    )
```

```python
import jax
import jax.numpy as jnp
from jax import lax
from jax.experimental import pallas as pl
from jax.experimental.pallas import tpu as pltpu
from jax.sharding import Mesh, PartitionSpec as P


BF = jnp.bfloat16
F32 = jnp.float32
NAMES = ("y", "zl", "core", "zh", "x")
BAND = ("y", "zl", "core")
SHARD = ("zh", "x")
N = 4
BANDS = 16
LANES = 128
DOWN = 1408
UP = 1536
Shape = jax.ShapeDtypeStruct


def spread(value, axis):
    return lax.all_to_all(jnp.broadcast_to(value[None], (N, *value.shape)), axis, 0, 0)


def pull(value, axis, step):
    return lax.ppermute(value, axis, [(i, (i - step) % N) for i in range(N)])


def gather_ring(value, axis):
    half = value.shape[0] // 2
    plus = pull(value, axis, 1)
    minus = pull(value, axis, -1)
    far_a = pull(plus[:half], axis, 1)
    far_b = pull(minus[half:], axis, -1)
    return value, plus, far_a, far_b, minus


def reduce_ring(blocks, axis):
    own, plus, two, minus = blocks
    half = own.shape[0] // 2
    far_a = pull(two[:half], axis, -1)
    far_b = pull(two[half:], axis, 1)
    plus = jnp.concatenate([(plus[:half].astype(F32) + far_a.astype(F32)).astype(BF), plus[half:]], 0)
    minus = jnp.concatenate([minus[:half], (minus[half:].astype(F32) + far_b.astype(F32)).astype(BF)], 0)
    plus = pull(plus, axis, -1)
    minus = pull(minus, axis, 1)
    return (own.astype(F32) + plus.astype(F32) + minus.astype(F32)).astype(BF)


def forward_kernel(
    at_ref, near_ref, near2_ref, far_ref, far2_ref, enc_ref, bias_ref, dec_ref, a_ref, linear_ref, active_ref, first_ref, second_ref
):
    half = near_ref.shape[1] // N

    def lay(mine, other):
        for z in range(N):
            a_ref[2 * half * z : 2 * half * z + half] = mine[0, half * z : half * z + half]
            a_ref[2 * half * z + half : 2 * half * z + 2 * half] = other[0, half * z : half * z + half]

    @pl.when(pl.program_id(0) != 2)
    def _():
        lay(near_ref, near2_ref)

    @pl.when(pl.program_id(0) == 2)
    def _():
        lay(far_ref, far2_ref)

    preact = jnp.dot(a_ref[...], enc_ref[...], preferred_element_type=F32) + bias_ref[...]
    linear = jnp.maximum(preact, 0.0)
    linear_ref[...] = linear
    active_ref[...] = (linear * linear).astype(BF)
    term = jnp.dot(active_ref[...], dec_ref[...], preferred_element_type=F32).astype(BF)
    for z in range(N):
        rows = slice(2 * half * z, 2 * half * z + 2 * half)
        place = pl.multiple_of(2 * half * ((at_ref[1] + z) % N), 2 * half)
        first_ref[0, pl.ds(place, 2 * half)] = term[rows, :DOWN]
        second_ref[z, 0] = term[rows, DOWN:]


def backward_kernel(
    at_ref, a0, a1, a2, a3, a4, b0, b1, b2, b3, b4, dec_ref, linear_ref, active_any, gathered_any,
    enc_out, dec_out, found_ref, up_ref, grad_ref, active_ref, gathered_ref, sems,
):
    block = a0.shape[0]
    rows = block // N
    width = up_ref.shape[1]
    rest = width - UP
    copies = [
        pltpu.make_async_copy(active_any, active_ref, sems.at[0]),
        pltpu.make_async_copy(gathered_any, gathered_ref, sems.at[1]),
    ]
    for copy in copies:
        copy.start()
    for x, pieces in enumerate(((a0,), (a1,), (a2, a3), (a4,))):
        z = 0
        for piece in pieces:
            for i in range(piece.shape[0] // rows):
                place = block * x + rows * ((z + N - at_ref[1]) % N)
                up_ref[pl.ds(pl.multiple_of(place, rows), rows), :UP] = piece[rows * i : rows * i + rows]
                z += 1
    found = jnp.zeros((8, LANES), F32)
    for z, pieces in enumerate(((b0,), (b1,), (b2, b3), (b4,))):
        x = 0
        for piece in pieces:
            for i in range(piece.shape[0] // rows):
                place = block * x + rows * z
                up_ref[place : place + rows, UP:] = piece[rows * i : rows * i + rows, :rest]
                found = found + piece[rows * i : rows * i + 8, rest:].astype(F32)
                x += 1
    found_ref[...] = found

    def first(x, _):
        span = pl.ds(pl.multiple_of(block * x, block), block)
        grads = lax.dot_general(up_ref[span], dec_ref[...], (((1,), (1,)), ((), ())), preferred_element_type=F32)
        grad_ref[span] = (2.0 * linear_ref[span] * grads).astype(BF)
        return 0

    lax.fori_loop(0, N, first, 0)
    contract = (((0,), (0,)), ((), ()))
    copies[0].wait()
    step = 2 * LANES

    def second(i, _):
        span = pl.ds(pl.multiple_of(step * i, step), step)
        dec_out[:, span] = lax.dot_general(
            active_ref[...], up_ref[:, span], contract, preferred_element_type=F32
        ).astype(BF)
        return 0

    lax.fori_loop(0, width // step, second, 0)
    copies[1].wait()

    def third(i, _):
        span = pl.ds(pl.multiple_of(step * i, step), step)
        enc_out[span] = lax.dot_general(
            gathered_ref[:, span], grad_ref[...], contract, preferred_element_type=F32
        ).astype(BF)
        return 0

    lax.fori_loop(0, width // step, third, 0)


def deal_kernel(core_ref, a_ref, b0, b1, b2, b3, dealt_ref):
    wide = dealt_ref.shape[2]
    cut = a_ref.shape[2] - wide
    part_a = jnp.sum(a_ref[...].astype(F32), axis=0).astype(dealt_ref.dtype)
    part_b = b0[...].astype(F32) + b1[...].astype(F32) + b2[...].astype(F32) + b3[...].astype(F32)
    part_b = part_b.astype(dealt_ref.dtype)
    flip = core_ref[0] * (BANDS // 4)
    for k in range(BANDS // 2):
        to = 2 * (k ^ flip)
        dealt_ref[to] = part_a[8 * k : 8 * k + 8, :wide]
        dealt_ref[to + 1, :, :cut] = part_a[8 * k : 8 * k + 8, wide:]
        dealt_ref[to + 1, :, cut:] = part_b[8 * k : 8 * k + 8]


def as_rows(found):
    high = found.astype(BF).astype(F32)
    low = found - high
    row = lax.broadcasted_iota(jnp.int32, (8, LANES), 0)
    return jnp.where(row == 0, high, jnp.where(row == 1, low, 0.0)).astype(BF)


def band_kernel(mixed_ref, local_ref, up_ref):
    wide = local_ref.shape[1]
    lane = lax.broadcasted_iota(jnp.int32, (1, LANES), 1)
    found = jnp.zeros((1, LANES), F32)
    error = local_ref[...].astype(F32)
    suffix = jnp.zeros_like(error)
    errors = []
    for k in range(BANDS):
        error = error - mixed_ref[k].astype(F32)
        errors.append(error)
        found = jnp.where(lane == k, jnp.sum(error * error), found)
    for k in reversed(range(BANDS)):
        suffix = suffix + errors[k]
        up_ref[k, :, :wide] = (suffix * (-1.0 / BANDS)).astype(BF)
    extra = as_rows(found)
    for k in range(BANDS):
        up_ref[k, :, wide:] = extra


def sort_kernel(core_ref, mixed_ref, up_a_ref, up_b_ref):
    wide = mixed_ref.shape[2] - LANES
    cut = UP - wide
    rest = 2 * wide - UP
    found = jnp.zeros((1, LANES), F32)
    flip = core_ref[0] * (BANDS // 4)
    up_b_ref[:, rest:] = jnp.zeros((up_b_ref.shape[0], LANES), BF)
    for k in range(BANDS // 2):
        rows = pl.ds(8 * k, 8)
        at = 2 * (k ^ flip)
        up_a_ref[rows, :wide] = mixed_ref[at, :, :wide]
        up_a_ref[rows, wide:] = mixed_ref[at + 1, :, :cut]
        up_b_ref[rows, :rest] = mixed_ref[at + 1, :, cut:wide]
    for k in range(BANDS):
        found = found + jnp.sum(mixed_ref[k, :, wide:].astype(F32), axis=0, keepdims=True)
    up_b_ref[:8, rest:] = as_rows(found)


SCALAR = pl.BlockSpec(memory_space=pltpu.SMEM)
LOCAL = pl.BlockSpec(memory_space=pltpu.VMEM)


def step(activations, encoder, encoder_bias, decoder):
    rows, width = activations.shape
    latents = encoder.shape[1]
    half = rows // 2
    block = rows * N
    total = block * N
    divisor = total * width
    rest = width - UP
    core = lax.axis_index("core")
    band = lax.axis_index(BAND)
    which = core.astype(jnp.int32).reshape(1)

    at = jnp.stack([lax.axis_index("x"), lax.axis_index("zh")]).astype(jnp.int32)

    column = jnp.concatenate(gather_ring(lax.dynamic_slice_in_dim(activations, core * half, half, 0), "zh"), 0)
    own, plus, far_a, far_b, minus = gather_ring(column, "x")
    near = jnp.stack([own, plus, minus])
    far = jnp.concatenate([far_a, far_b], 0)[None]
    near2, far2 = [lax.ppermute(v, "core", [(0, 1), (1, 0)]) for v in (near, far)]

    fixed = lambda i, at: (0, 0)
    by_row = lambda i, at: (i, 0)
    by_near = lambda i, at: ((i + 1) // 2, 0, 0)
    by_far = lambda i, at: (0, 0, 0)
    gathered, linear, active, first, second = pl.pallas_call(
        forward_kernel,
        grid_spec=pltpu.PrefetchScalarGridSpec(
            num_scalar_prefetch=1,
            grid=(N,),
            in_specs=[
                pl.BlockSpec((1, block // 2, width), by_near),
                pl.BlockSpec((1, block // 2, width), by_near),
                pl.BlockSpec((1, block // 2, width), by_far),
                pl.BlockSpec((1, block // 2, width), by_far),
                pl.BlockSpec((width, latents), fixed),
                pl.BlockSpec((1, latents), fixed),
                pl.BlockSpec((latents, width), fixed),
            ],
            out_specs=[
                pl.BlockSpec((block, width), by_row),
                pl.BlockSpec((block, latents), by_row),
                pl.BlockSpec((block, latents), by_row),
                pl.BlockSpec((1, block, DOWN), lambda i, at: (i, 0, 0)),
                pl.BlockSpec((N, 1, rows, width - DOWN), lambda i, at: (0, i, 0, 0)),
            ],
        ),
        out_shape=[
            Shape((total, width), BF),
            Shape((total, latents), F32),
            Shape((total, latents), BF),
            Shape((N, block, DOWN), BF),
            Shape((N, N, rows, width - DOWN), BF),
        ],
    )(at, near, near2, far, far2, encoder, encoder_bias.reshape(1, latents), decoder)

    first = reduce_ring(first, "x")
    second = reduce_ring(second.reshape(N, block, width - DOWN), "zh")
    first = lax.all_to_all(first.reshape(N, rows, DOWN), "zh", 0, 0)
    second = [second[o * rows : (o + 1) * rows] for o in range(N)]
    second = [second[0]] + [pull(second[o], "x", -o) for o in range(1, N)]

    wide = width // 2
    dealt = pl.pallas_call(
        deal_kernel,
        out_shape=Shape((BANDS, 8, wide), BF),
        in_specs=[SCALAR] + [LOCAL] * 5,
        out_specs=LOCAL,
    )(which, first, *second)
    mixed = lax.all_to_all(dealt, BAND, 0, 0)
    local = lax.dynamic_slice(activations, (8 * (band // 2), wide * (band % 2)), (8, wide))
    ups = pl.pallas_call(
        band_kernel,
        out_shape=Shape((BANDS, 8, wide + LANES), BF),
        in_specs=[LOCAL, LOCAL],
        out_specs=LOCAL,
    )(mixed, local)
    ups = lax.all_to_all(ups, BAND, 0, 0)
    up_a, up_b = pl.pallas_call(
        sort_kernel,
        out_shape=[Shape((rows, UP), BF), Shape((rows, rest + LANES), BF)],
        in_specs=[SCALAR, LOCAL],
        out_specs=[LOCAL, LOCAL],
    )(which, ups)

    others = [pull(up_b, "x", o) for o in range(1, N)]
    up_b = jnp.concatenate([up_b] + others, 0)
    up_a = spread(up_a, "zh")
    up_a = gather_ring(up_a.reshape(block, UP), "x")
    up_b = gather_ring(up_b, "zh")

    anywhere = pl.BlockSpec(memory_space=pl.ANY)
    enc_grads, dec_grads, found = pl.pallas_call(
        backward_kernel,
        in_specs=[SCALAR] + [LOCAL] * 12 + [anywhere] * 2,
        out_specs=[LOCAL] * 3,
        out_shape=[Shape((width, latents), BF), Shape((latents, width), BF), Shape((8, LANES), F32)],
        scratch_shapes=[
            pltpu.VMEM((total, width), BF),
            pltpu.VMEM((total, latents), BF),
            pltpu.VMEM((total, latents), BF),
            pltpu.VMEM((total, width), BF),
            pltpu.SemaphoreType.DMA((2,)),
        ],
    )(at, *up_a, *up_b, decoder, linear, active, gathered)
    losses = jnp.sum(found, axis=0)[:BANDS] / divisor
    return losses, enc_grads, dec_grads


def solution(mesh):
    grid = Mesh(mesh.devices.reshape(4, 2, 2, 4, 4), NAMES)
    both = BAND + SHARD
    return jax.shard_map(
        step,
        mesh=grid,
        in_specs=(P(SHARD, None), P(None, both), P(both), P(both, None)),
        out_specs=(P(), P(None, both), P(both, None)),
        check_vma=False,
    )
```

```python
import jax
import jax.numpy as jnp
from jax import lax
from jax.experimental import pallas as pl
from jax.experimental.pallas import tpu as pltpu
from jax.sharding import Mesh, PartitionSpec as P


BF = jnp.bfloat16
F32 = jnp.float32
NAMES = ("y", "zl", "core", "zh", "x")
BAND = ("y", "zl", "core")
SHARD = ("zh", "x")
N = 4
BANDS = 16
LANES = 128
DOWN = 1536
UP = 1536
Shape = jax.ShapeDtypeStruct


def pull(value, axis, step):
    return lax.ppermute(value, axis, [(i, (i - step) % N) for i in range(N)])


def gather_ring(value, axis):
    half = value.shape[0] // 2
    plus = pull(value, axis, 1)
    minus = pull(value, axis, -1)
    far_a = pull(plus[:half], axis, 1)
    far_b = pull(minus[half:], axis, -1)
    return value, plus, far_a, far_b, minus


def reduce_ring(blocks, axis):
    own, plus, two, minus = blocks
    half = own.shape[0] // 2
    far_a = pull(two[:half], axis, -1)
    far_b = pull(two[half:], axis, 1)
    plus = jnp.concatenate([(plus[:half].astype(F32) + far_a.astype(F32)).astype(BF), plus[half:]], 0)
    minus = jnp.concatenate([minus[:half], (minus[half:].astype(F32) + far_b.astype(F32)).astype(BF)], 0)
    plus = pull(plus, axis, -1)
    minus = pull(minus, axis, 1)
    return (own.astype(F32) + plus.astype(F32) + minus.astype(F32)).astype(BF)


def forward_kernel(
    at_ref, near_ref, near2_ref, far_ref, far2_ref, enc_ref, bias_ref, dec_ref, a_ref, linear_ref, active_ref, first_ref, second_ref
):
    half = near_ref.shape[1] // N

    def lay(mine, other):
        for z in range(N):
            a_ref[2 * half * z : 2 * half * z + half] = mine[0, half * z : half * z + half]
            a_ref[2 * half * z + half : 2 * half * z + 2 * half] = other[0, half * z : half * z + half]

    @pl.when(pl.program_id(0) != 2)
    def _():
        lay(near_ref, near2_ref)

    @pl.when(pl.program_id(0) == 2)
    def _():
        lay(far_ref, far2_ref)

    preact = jnp.dot(a_ref[...], enc_ref[...], preferred_element_type=F32) + bias_ref[...]
    linear = jnp.maximum(preact, 0.0)
    linear_ref[...] = linear
    active_ref[...] = (linear * linear).astype(BF)
    term = jnp.dot(active_ref[...], dec_ref[...], preferred_element_type=F32).astype(BF)
    for z in range(N):
        rows = slice(2 * half * z, 2 * half * z + 2 * half)
        place = pl.multiple_of(2 * half * ((at_ref[1] + z) % N), 2 * half)
        first_ref[0, pl.ds(place, 2 * half)] = term[rows, :DOWN]
        second_ref[z, 0] = term[rows, DOWN:]


def backward_kernel(
    a0, a1, a2, a3, a4, b0, b1, b2, b3, b4, dec_any, linear_any, active_any, gathered_any,
    enc_out, dec_out, found_ref, up_ref, extra_ref, grad_ref, dec_ref, linear_ref, active_ref, gathered_ref, sems, up_sems,
):
    block = a0.shape[0]
    rows = block // N
    width = up_ref.shape[1]
    rest = width - UP

    def fetch(source, target, sem):
        copy = pltpu.make_async_copy(source, target, sem)
        copy.start()
        return copy

    whole = [fetch(dec_any, dec_ref, sems.at[0])]
    parts = []
    for x in range(N):
        here, at = [], block * x
        for piece in ((a0,), (a1,), (a2, a3), (a4,))[x]:
            size = piece.shape[0]
            here.append(fetch(piece, up_ref.at[at : at + size, :UP], up_sems.at[x, len(here)]))
            at += size
        for z in range(N):
            piece, i = ((b0, x), (b1, x), (b2, x) if x < 2 else (b3, x - 2), (b4, x))[z]
            at = block * x + rows * z
            source = piece.at[rows * i : rows * i + rows]
            here.append(fetch(source.at[:, :rest], up_ref.at[at : at + rows, UP:], up_sems.at[x, len(here)]))
            here.append(fetch(source.at[:, rest:], extra_ref.at[at : at + rows], up_sems.at[x, len(here)]))
        parts.append(here)
        if x == 0:
            whole.append(fetch(linear_any, linear_ref, sems.at[1]))
    whole.append(fetch(active_any, active_ref, sems.at[2]))
    whole.append(fetch(gathered_any, gathered_ref, sems.at[3]))
    whole[0].wait()
    whole[1].wait()

    def first(x, _):
        for k in range(N):

            @pl.when(x == k)
            def _():
                for copy in parts[k]:
                    copy.wait()

        span = pl.ds(pl.multiple_of(block * x, block), block)
        grads = lax.dot_general(up_ref[span], dec_ref[...], (((1,), (1,)), ((), ())), preferred_element_type=F32)
        grad_ref[span] = (2.0 * linear_ref[span] * grads).astype(BF)
        return 0

    lax.fori_loop(0, N, first, 0)
    found = jnp.zeros((8, LANES), F32)
    for i in range(N * N):
        found = found + extra_ref[rows * i : rows * i + 8].astype(F32)
    found_ref[...] = jnp.sum(found, axis=0, keepdims=True)

    contract = (((0,), (0,)), ((), ()))
    step = 2 * LANES
    whole[2].wait()

    def second(i, _):
        span = pl.ds(pl.multiple_of(step * i, step), step)
        dec_out[span] = lax.dot_general(
            active_ref[:, span], up_ref[...], contract, preferred_element_type=F32
        ).astype(BF)
        return 0

    lax.fori_loop(0, active_ref.shape[1] // step, second, 0)
    whole[3].wait()

    def third(i, _):
        span = pl.ds(pl.multiple_of(step * i, step), step)
        enc_out[span] = lax.dot_general(
            gathered_ref[:, span], grad_ref[...], contract, preferred_element_type=F32
        ).astype(BF)
        return 0

    lax.fori_loop(0, width // step, third, 0)


def deal_kernel(core_ref, a_ref, b0, b1, b2, b3, dealt_ref):
    wide = dealt_ref.shape[2]
    cut = a_ref.shape[2] - wide
    part_a = jnp.sum(a_ref[...].astype(F32), axis=0).astype(dealt_ref.dtype)
    part_b = b0[...].astype(F32) + b1[...].astype(F32) + b2[...].astype(F32) + b3[...].astype(F32)
    part_b = part_b.astype(dealt_ref.dtype)
    flip = core_ref[0] * (BANDS // 4)
    for k in range(BANDS // 2):
        to = 2 * (k ^ flip)
        dealt_ref[to] = part_a[8 * k : 8 * k + 8, :wide]
        dealt_ref[to + 1, :, :cut] = part_a[8 * k : 8 * k + 8, wide:]
        dealt_ref[to + 1, :, cut:] = part_b[8 * k : 8 * k + 8]


def as_rows(found):
    high = found.astype(BF).astype(F32)
    low = found - high
    row = lax.broadcasted_iota(jnp.int32, (8, LANES), 0)
    return jnp.where(row == 0, high, jnp.where(row == 1, low, 0.0)).astype(BF)


def band_kernel(mixed_ref, local_ref, up_ref):
    wide = local_ref.shape[1]
    lane = lax.broadcasted_iota(jnp.int32, (1, LANES), 1)
    found = jnp.zeros((1, LANES), F32)
    error = local_ref[...].astype(F32)
    suffix = jnp.zeros_like(error)
    errors = []
    for k in range(BANDS):
        error = error - mixed_ref[k].astype(F32)
        errors.append(error)
        found = jnp.where(lane == k, jnp.sum(error * error), found)
    for k in reversed(range(BANDS)):
        suffix = suffix + errors[k]
        up_ref[k, :, :wide] = (suffix * (-1.0 / BANDS)).astype(BF)
    extra = as_rows(found)
    for k in range(BANDS):
        up_ref[k, :, wide:] = extra


def sort_kernel(core_ref, mixed_ref, up_a_ref, up_b_ref):
    wide = mixed_ref.shape[2] - LANES
    cut = UP - wide
    rest = 2 * wide - UP
    found = jnp.zeros((1, LANES), F32)
    flip = core_ref[0] * (BANDS // 4)
    up_b_ref[:, rest:] = jnp.zeros((up_b_ref.shape[0], LANES), BF)
    for k in range(BANDS // 2):
        rows = pl.ds(8 * k, 8)
        at = 2 * (k ^ flip)
        up_a_ref[rows, :wide] = mixed_ref[at, :, :wide]
        up_a_ref[rows, wide:] = mixed_ref[at + 1, :, :cut]
        up_b_ref[rows, :rest] = mixed_ref[at + 1, :, cut:wide]
    for k in range(BANDS):
        found = found + jnp.sum(mixed_ref[k, :, wide:].astype(F32), axis=0, keepdims=True)
    up_b_ref[:8, rest:] = as_rows(found)


SCALAR = pl.BlockSpec(memory_space=pltpu.SMEM)
LOCAL = pl.BlockSpec(memory_space=pltpu.VMEM)


def step(activations, encoder, encoder_bias, decoder):
    rows, width = activations.shape
    latents = encoder.shape[1]
    half = rows // 2
    block = rows * N
    total = block * N
    divisor = total * width
    rest = width - UP
    core = lax.axis_index("core")
    band = lax.axis_index(BAND)
    which = core.astype(jnp.int32).reshape(1)

    at = jnp.stack([lax.axis_index("x"), lax.axis_index("zh")]).astype(jnp.int32)

    column = jnp.concatenate(gather_ring(lax.dynamic_slice_in_dim(activations, core * half, half, 0), "zh"), 0)
    own, plus, far_a, far_b, minus = gather_ring(column, "x")
    near = jnp.stack([own, plus, minus])
    far = jnp.concatenate([far_a, far_b], 0)[None]
    near2, far2 = [lax.ppermute(v, "core", [(0, 1), (1, 0)]) for v in (near, far)]

    fixed = lambda i, at: (0, 0)
    by_row = lambda i, at: (i, 0)
    by_near = lambda i, at: ((i + 1) // 2, 0, 0)
    by_far = lambda i, at: (0, 0, 0)
    gathered, linear, active, first, second = pl.pallas_call(
        forward_kernel,
        grid_spec=pltpu.PrefetchScalarGridSpec(
            num_scalar_prefetch=1,
            grid=(N,),
            in_specs=[
                pl.BlockSpec((1, block // 2, width), by_near),
                pl.BlockSpec((1, block // 2, width), by_near),
                pl.BlockSpec((1, block // 2, width), by_far),
                pl.BlockSpec((1, block // 2, width), by_far),
                pl.BlockSpec((width, latents), fixed),
                pl.BlockSpec((1, latents), fixed),
                pl.BlockSpec((latents, width), fixed),
            ],
            out_specs=[
                pl.BlockSpec((block, width), by_row),
                pl.BlockSpec((block, latents), by_row),
                pl.BlockSpec((block, latents), by_row),
                pl.BlockSpec((1, block, DOWN), lambda i, at: (i, 0, 0)),
                pl.BlockSpec((N, 1, rows, width - DOWN), lambda i, at: (0, i, 0, 0)),
            ],
        ),
        out_shape=[
            Shape((total, width), BF),
            Shape((total, latents), F32),
            Shape((total, latents), BF),
            Shape((N, block, DOWN), BF),
            Shape((N, N, rows, width - DOWN), BF),
        ],
    )(at, near, near2, far, far2, encoder, encoder_bias.reshape(1, latents), decoder)

    first = reduce_ring(first, "x")
    second = reduce_ring(second.reshape(N, block, width - DOWN), "zh")
    first = lax.all_to_all(first.reshape(N, rows, DOWN), "zh", 0, 0)
    second = [second[o * rows : (o + 1) * rows] for o in range(N)]
    second = [second[0]] + [pull(second[o], "x", -o) for o in range(1, N)]

    wide = width // 2
    dealt = pl.pallas_call(
        deal_kernel,
        out_shape=Shape((BANDS, 8, wide), BF),
        in_specs=[SCALAR] + [LOCAL] * 5,
        out_specs=LOCAL,
    )(which, first, *second)
    mixed = lax.all_to_all(dealt, BAND, 0, 0)
    local = lax.dynamic_slice(activations, (8 * (band // 2), wide * (band % 2)), (8, wide))
    ups = pl.pallas_call(
        band_kernel,
        out_shape=Shape((BANDS, 8, wide + LANES), BF),
        in_specs=[LOCAL, LOCAL],
        out_specs=LOCAL,
    )(mixed, local)
    ups = lax.all_to_all(ups, BAND, 0, 0)
    up_a, up_b = pl.pallas_call(
        sort_kernel,
        out_shape=[Shape((rows, UP), BF), Shape((rows, rest + LANES), BF)],
        in_specs=[SCALAR, LOCAL],
        out_specs=[LOCAL, LOCAL],
    )(which, ups)

    up_a = jnp.concatenate(gather_ring(up_a, "zh"), 0)
    others = [pull(up_b, "x", o) for o in range(1, N)]
    up_b = jnp.concatenate([up_b] + others, 0)
    up_a = gather_ring(up_a, "x")
    up_b = gather_ring(up_b, "zh")

    anywhere = pl.BlockSpec(memory_space=pl.ANY)
    enc_grads, dec_grads, found = pl.pallas_call(
        backward_kernel,
        in_specs=[anywhere] * 14,
        out_specs=[LOCAL] * 3,
        out_shape=[Shape((width, latents), BF), Shape((latents, width), BF), Shape((1, LANES), F32)],
        scratch_shapes=[
            pltpu.VMEM((total, width), BF),
            pltpu.VMEM((total, LANES), BF),
            pltpu.VMEM((total, latents), BF),
            pltpu.VMEM((latents, width), BF),
            pltpu.VMEM((total, latents), F32),
            pltpu.VMEM((total, latents), BF),
            pltpu.VMEM((total, width), BF),
            pltpu.SemaphoreType.DMA((4,)),
            pltpu.SemaphoreType.DMA((N, 2 + 2 * N)),
        ],
    )(*up_a, *up_b, decoder, linear, active, gathered)
    losses = found[0, :BANDS] / divisor
    return losses, enc_grads, dec_grads


def solution(mesh):
    grid = Mesh(mesh.devices.reshape(4, 2, 2, 4, 4), NAMES)
    both = BAND + SHARD
    return jax.shard_map(
        step,
        mesh=grid,
        in_specs=(P(SHARD, None), P(None, both), P(both), P(both, None)),
        out_specs=(P(), P(None, both), P(both, None)),
        check_vma=False,
    )
```

```python
import jax
import jax.numpy as jnp
from jax import lax
from jax.experimental import pallas as pl
from jax.experimental.pallas import tpu as pltpu
from jax.sharding import Mesh, PartitionSpec as P


BF = jnp.bfloat16
F32 = jnp.float32
NAMES = ("y", "zl", "core", "zh", "x")
BAND = ("y", "zl", "core")
SHARD = ("zh", "x")
N = 4
BANDS = 16
LANES = 128
DOWN = 1408
UP = 1536
Shape = jax.ShapeDtypeStruct


def pull(value, axis, step):
    return lax.ppermute(value, axis, [(i, (i - step) % N) for i in range(N)])


def gather_ring(value, axis):
    half = value.shape[0] // 2
    plus = pull(value, axis, 1)
    minus = pull(value, axis, -1)
    far_a = pull(plus[:half], axis, 1)
    far_b = pull(minus[half:], axis, -1)
    return value, plus, far_a, far_b, minus


def reduce_ring(blocks, axis):
    own, plus, two, minus = blocks
    half = own.shape[0] // 2
    far_a = pull(two[:half], axis, -1)
    far_b = pull(two[half:], axis, 1)
    plus = jnp.concatenate([(plus[:half].astype(F32) + far_a.astype(F32)).astype(BF), plus[half:]], 0)
    minus = jnp.concatenate([minus[:half], (minus[half:].astype(F32) + far_b.astype(F32)).astype(BF)], 0)
    plus = pull(plus, axis, -1)
    minus = pull(minus, axis, 1)
    return (own.astype(F32) + plus.astype(F32) + minus.astype(F32)).astype(BF)


def forward_kernel(
    at_ref, near_ref, near2_ref, far_ref, far2_ref, enc_ref, bias_ref, dec_ref, a_ref, linear_ref, active_ref, first_ref, second_ref
):
    half = near_ref.shape[1] // N

    def lay(mine, other):
        for z in range(N):
            a_ref[2 * half * z : 2 * half * z + half] = mine[0, half * z : half * z + half]
            a_ref[2 * half * z + half : 2 * half * z + 2 * half] = other[0, half * z : half * z + half]

    @pl.when(pl.program_id(0) != 2)
    def _():
        lay(near_ref, near2_ref)

    @pl.when(pl.program_id(0) == 2)
    def _():
        lay(far_ref, far2_ref)

    preact = jnp.dot(a_ref[...], enc_ref[...], preferred_element_type=F32) + bias_ref[...]
    linear = jnp.maximum(preact, 0.0)
    linear_ref[...] = linear
    active_ref[...] = (linear * linear).astype(BF)
    term = jnp.dot(active_ref[...], dec_ref[...], preferred_element_type=F32).astype(BF)
    for z in range(N):
        rows = slice(2 * half * z, 2 * half * z + 2 * half)
        place = pl.multiple_of(2 * half * ((at_ref[1] + z) % N), 2 * half)
        first_ref[0, pl.ds(place, 2 * half)] = term[rows, :DOWN]
        second_ref[z, 0] = term[rows, DOWN:]


def backward_kernel(
    a0, a1, a2, a3, a4, b0, b1, b2, b3, b4, dec_any, linear_any, active_any, gathered_any,
    enc_out, dec_out, found_ref, up_ref, extra_ref, grad_ref, dec_ref, linear_ref, active_ref, gathered_ref, turned_ref, sems, up_sems,
):
    block = a0.shape[0]
    rows = block // N
    width = up_ref.shape[1]
    rest = width - UP

    def fetch(source, target, sem):
        copy = pltpu.make_async_copy(source, target, sem)
        copy.start()
        return copy

    whole = [fetch(dec_any, dec_ref, sems.at[0])]
    parts = []
    for x in range(N):
        here, at = [], block * x
        for piece in ((a0,), (a1,), (a2, a3), (a4,))[x]:
            size = piece.shape[0]
            here.append(fetch(piece, up_ref.at[at : at + size, :UP], up_sems.at[x, len(here)]))
            at += size
        for z in range(N):
            piece, i = ((b0, x), (b1, x), (b2, x) if x < 2 else (b3, x - 2), (b4, x))[z]
            at = block * x + rows * z
            source = piece.at[rows * i : rows * i + rows]
            here.append(fetch(source.at[:, :rest], up_ref.at[at : at + rows, UP:], up_sems.at[x, len(here)]))
            here.append(fetch(source.at[:, rest:], extra_ref.at[at : at + rows], up_sems.at[x, len(here)]))
        parts.append(here)
        if x == 0:
            whole.append(fetch(linear_any, linear_ref, sems.at[1]))
    whole.append(fetch(active_any, active_ref, sems.at[2]))
    whole.append(fetch(gathered_any, gathered_ref, sems.at[3]))
    whole[0].wait()
    whole[1].wait()

    def first(x, _):
        for k in range(N):

            @pl.when(x == k // 2)
            def _():
                for copy in parts[k]:
                    copy.wait()

        span = pl.ds(pl.multiple_of(2 * block * x, 2 * block), 2 * block)
        grads = lax.dot_general(up_ref[span], dec_ref[...], (((1,), (1,)), ((), ())), preferred_element_type=F32)
        grad_ref[span] = (2.0 * linear_ref[span] * grads).astype(BF)
        return 0

    lax.fori_loop(0, N // 2, first, 0)
    found = jnp.zeros((8, LANES), F32)
    for i in range(N * N):
        found = found + extra_ref[rows * i : rows * i + 8].astype(F32)
    found_ref[...] = jnp.sum(found, axis=0, keepdims=True)

    contract = (((0,), (0,)), ((), ()))
    step = 2 * LANES
    whole[2].wait()

    turned_ref[...] = active_ref[...].T

    def second(i, _):
        span = pl.ds(pl.multiple_of(step * i, step), step)
        dec_out[:, span] = jnp.dot(turned_ref[...], up_ref[:, span], preferred_element_type=F32).astype(BF)
        return 0

    lax.fori_loop(0, width // step, second, 0)
    tall = 3 * step
    whole[3].wait()

    def third(i, _):
        span = pl.ds(pl.multiple_of(tall * i, tall), tall)
        enc_out[span] = lax.dot_general(
            gathered_ref[:, span], grad_ref[...], contract, preferred_element_type=F32
        ).astype(BF)
        return 0

    lax.fori_loop(0, width // tall, third, 0)


def deal_kernel(core_ref, a_ref, b0, b1, b2, b3, dealt_ref):
    wide = dealt_ref.shape[2]
    cut = a_ref.shape[2] - wide
    part_a = jnp.sum(a_ref[...].astype(F32), axis=0).astype(dealt_ref.dtype)
    part_b = b0[...].astype(F32) + b1[...].astype(F32) + b2[...].astype(F32) + b3[...].astype(F32)
    part_b = part_b.astype(dealt_ref.dtype)
    flip = core_ref[0] * (BANDS // 4)
    for k in range(BANDS // 2):
        to = 2 * (k ^ flip)
        dealt_ref[to] = part_a[8 * k : 8 * k + 8, :wide]
        dealt_ref[to + 1, :, :cut] = part_a[8 * k : 8 * k + 8, wide:]
        dealt_ref[to + 1, :, cut:] = part_b[8 * k : 8 * k + 8]


def as_rows(found):
    high = found.astype(BF).astype(F32)
    low = found - high
    row = lax.broadcasted_iota(jnp.int32, (8, LANES), 0)
    return jnp.where(row == 0, high, jnp.where(row == 1, low, 0.0)).astype(BF)


def band_kernel(mixed_ref, local_ref, up_ref):
    wide = local_ref.shape[1]
    lane = lax.broadcasted_iota(jnp.int32, (1, LANES), 1)
    found = jnp.zeros((1, LANES), F32)
    error = local_ref[...].astype(F32)
    suffix = jnp.zeros_like(error)
    errors = []
    for k in range(BANDS):
        error = error - mixed_ref[k].astype(F32)
        errors.append(error)
        found = jnp.where(lane == k, jnp.sum(error * error), found)
    for k in reversed(range(BANDS)):
        suffix = suffix + errors[k]
        up_ref[k, :, :wide] = (suffix * (-1.0 / BANDS)).astype(BF)
    extra = as_rows(found)
    for k in range(BANDS):
        up_ref[k, :, wide:] = extra


def sort_kernel(core_ref, mixed_ref, up_a_ref, up_b_ref):
    wide = mixed_ref.shape[2] - LANES
    cut = UP - wide
    rest = 2 * wide - UP
    found = jnp.zeros((1, LANES), F32)
    flip = core_ref[0] * (BANDS // 4)
    up_b_ref[:, rest:] = jnp.zeros((up_b_ref.shape[0], LANES), BF)
    for k in range(BANDS // 2):
        rows = pl.ds(8 * k, 8)
        at = 2 * (k ^ flip)
        up_a_ref[rows, :wide] = mixed_ref[at, :, :wide]
        up_a_ref[rows, wide:] = mixed_ref[at + 1, :, :cut]
        up_b_ref[rows, :rest] = mixed_ref[at + 1, :, cut:wide]
    for k in range(BANDS):
        found = found + jnp.sum(mixed_ref[k, :, wide:].astype(F32), axis=0, keepdims=True)
    up_b_ref[:8, rest:] = as_rows(found)


SCALAR = pl.BlockSpec(memory_space=pltpu.SMEM)
LOCAL = pl.BlockSpec(memory_space=pltpu.VMEM)


def step(activations, encoder, encoder_bias, decoder):
    rows, width = activations.shape
    latents = encoder.shape[1]
    half = rows // 2
    block = rows * N
    total = block * N
    divisor = total * width
    rest = width - UP
    core = lax.axis_index("core")
    band = lax.axis_index(BAND)
    which = core.astype(jnp.int32).reshape(1)

    at = jnp.stack([lax.axis_index("x"), lax.axis_index("zh")]).astype(jnp.int32)

    column = jnp.concatenate(gather_ring(lax.dynamic_slice_in_dim(activations, core * half, half, 0), "zh"), 0)
    own, plus, far_a, far_b, minus = gather_ring(column, "x")
    near = jnp.stack([own, plus, minus])
    far = jnp.concatenate([far_a, far_b], 0)[None]
    near2, far2 = [lax.ppermute(v, "core", [(0, 1), (1, 0)]) for v in (near, far)]

    fixed = lambda i, at: (0, 0)
    by_row = lambda i, at: (i, 0)
    by_near = lambda i, at: ((i + 1) // 2, 0, 0)
    by_far = lambda i, at: (0, 0, 0)
    gathered, linear, active, first, second = pl.pallas_call(
        forward_kernel,
        grid_spec=pltpu.PrefetchScalarGridSpec(
            num_scalar_prefetch=1,
            grid=(N,),
            in_specs=[
                pl.BlockSpec((1, block // 2, width), by_near),
                pl.BlockSpec((1, block // 2, width), by_near),
                pl.BlockSpec((1, block // 2, width), by_far),
                pl.BlockSpec((1, block // 2, width), by_far),
                pl.BlockSpec((width, latents), fixed),
                pl.BlockSpec((1, latents), fixed),
                pl.BlockSpec((latents, width), fixed),
            ],
            out_specs=[
                pl.BlockSpec((block, width), by_row),
                pl.BlockSpec((block, latents), by_row),
                pl.BlockSpec((block, latents), by_row),
                pl.BlockSpec((1, block, DOWN), lambda i, at: (i, 0, 0)),
                pl.BlockSpec((N, 1, rows, width - DOWN), lambda i, at: (0, i, 0, 0)),
            ],
        ),
        out_shape=[
            Shape((total, width), BF),
            Shape((total, latents), F32),
            Shape((total, latents), BF),
            Shape((N, block, DOWN), BF),
            Shape((N, N, rows, width - DOWN), BF),
        ],
    )(at, near, near2, far, far2, encoder, encoder_bias.reshape(1, latents), decoder)

    first = reduce_ring(first, "x")
    second = reduce_ring(second.reshape(N, block, width - DOWN), "zh")
    first = lax.all_to_all(first.reshape(N, rows, DOWN), "zh", 0, 0)
    second = [second[o * rows : (o + 1) * rows] for o in range(N)]
    second = [second[0]] + [pull(second[o], "x", -o) for o in range(1, N)]

    wide = width // 2
    dealt = pl.pallas_call(
        deal_kernel,
        out_shape=Shape((BANDS, 8, wide), BF),
        in_specs=[SCALAR] + [LOCAL] * 5,
        out_specs=LOCAL,
    )(which, first, *second)
    mixed = lax.all_to_all(dealt, BAND, 0, 0)
    local = lax.dynamic_slice(activations, (8 * (band // 2), wide * (band % 2)), (8, wide))
    ups = pl.pallas_call(
        band_kernel,
        out_shape=Shape((BANDS, 8, wide + LANES), BF),
        in_specs=[LOCAL, LOCAL],
        out_specs=LOCAL,
    )(mixed, local)
    ups = lax.all_to_all(ups, BAND, 0, 0)
    up_a, up_b = pl.pallas_call(
        sort_kernel,
        out_shape=[Shape((rows, UP), BF), Shape((rows, rest + LANES), BF)],
        in_specs=[SCALAR, LOCAL],
        out_specs=[LOCAL, LOCAL],
    )(which, ups)

    up_a = jnp.concatenate(gather_ring(up_a, "zh"), 0)
    others = [pull(up_b, "x", o) for o in range(1, N)]
    up_b = jnp.concatenate([up_b] + others, 0)
    up_a = gather_ring(up_a, "x")
    up_b = gather_ring(up_b, "zh")

    anywhere = pl.BlockSpec(memory_space=pl.ANY)
    enc_grads, dec_grads, found = pl.pallas_call(
        backward_kernel,
        in_specs=[anywhere] * 14,
        out_specs=[LOCAL] * 3,
        out_shape=[Shape((width, latents), BF), Shape((latents, width), BF), Shape((1, LANES), F32)],
        scratch_shapes=[
            pltpu.VMEM((total, width), BF),
            pltpu.VMEM((total, LANES), BF),
            pltpu.VMEM((total, latents), BF),
            pltpu.VMEM((latents, width), BF),
            pltpu.VMEM((total, latents), F32),
            pltpu.VMEM((total, latents), BF),
            pltpu.VMEM((total, width), BF),
            pltpu.VMEM((latents, total), BF),
            pltpu.SemaphoreType.DMA((4,)),
            pltpu.SemaphoreType.DMA((N, 2 + 2 * N)),
        ],
    )(*up_a, *up_b, decoder, linear, active, gathered)
    losses = found[0, :BANDS] / divisor
    return losses, enc_grads, dec_grads


def solution(mesh):
    grid = Mesh(mesh.devices.reshape(4, 2, 2, 4, 4), NAMES)
    both = BAND + SHARD
    return jax.shard_map(
        step,
        mesh=grid,
        in_specs=(P(SHARD, None), P(None, both), P(both), P(both, None)),
        out_specs=(P(), P(None, both), P(both, None)),
        check_vma=False,
    )
```
